32 devices in a mesh: gx: 4 (over y, core), gy: 4 (over z), gz: 2 (over x).
Axes of the slice: x: 2, y: 2, z: 4, core: 2. Of those that a mesh axis runs over, the one named last changes fastest.
Arguments:
- positions: float32 [3, 4, 32, 2, 128], P(None, 'gx', ('gy', 'gz')), may hold values from 0 to 3
- velocities: float32 [3, 4, 32, 2, 128], P(None, 'gx', ('gy', 'gz')), may hold values from -6 to 6
- bead_keys: int32 [4, 32, 2, 128], P('gx', ('gy', 'gz')), may hold values from 0 to 1073741823
- counts: int32 [4, 32, 2], P('gx', ('gy', 'gz')), may hold values from 64 to 128
Outputs:
- half_kick: float32 [3, 4, 32, 2, 128], P(None, 'gx', 'gy', 'gz')
The draws below stay inside these ranges and needn't reach their ends.
Inputs may be any that keep to these rules, and one draw needn't show every extreme that they name: Slots from counts of a tile on are padding and take no part. `bead_keys`: the lowest bit of a key names the bead type, 0 water and 1 polymer.
All inputs are finite; a program needn't handle non-finite values.
Results may differ from the reference program's by a relative error of at most 0.0003.
Values sent between devices are 32-bit elements; how exact they have to be, the bound alone decides.
A program may use at most 64 MiB of HBM per device.

```python
import jax
import jax.numpy as jnp
from jax import lax

SLOTS = 128
SIDE = 3
NTX = 4
NTY = 32
NTZ = 2


def place_ends(values, own_key, smallest, top_value):
    index_at = [jax.random.randint(jax.random.fold_in(own_key, axis), (), 0, length) for axis, length in enumerate(values.shape)]
    main_axis = values.shape.index(max(values.shape))
    next_to = index_at[:main_axis] + [(index_at[main_axis] + 1) % values.shape[main_axis]] + index_at[main_axis + 1:]
    return values.at[tuple(index_at)].set(smallest).at[tuple(next_to)].set(top_value)


def levels(stream_key, shape, split, low, largest):
    def one(axis_at, blocks):
        heights = jax.random.uniform(jax.random.fold_in(jax.random.fold_in(stream_key, 6), axis_at), (blocks,), jnp.float32, low / len(split), largest / len(split))
        return jnp.repeat(jnp.exp(heights), shape[axis_at] // blocks).reshape((-1,) + (1,) * (len(shape) - axis_at - 1))

    factor_of = one(*split[0])
    for cut in split[1:]:
        factor_of = factor_of * one(*cut)
    return factor_of


def bell_draw(rng, extent, width, reach, split=(), kind=jnp.bfloat16):
    result = jax.random.normal(rng, extent, jnp.float32) * width
    if len(split) > 0:
        result = levels(rng, extent, split, -0.22, 0.18) * result
    return jnp.clip(result, min=-reach, max=reach).astype(kind)


def setup_inputs(seed: int = 0) -> dict:
    streams_of = jax.random.split(jax.random.key(seed), 5)
    return {
        "positions": jnp.clip(3.0 * jax.random.uniform(streams_of[0], (3, NTX, NTY, NTZ, SLOTS), jnp.float32) ** levels(streams_of[0], (3, NTX, NTY, NTZ, SLOTS), ((1, 4), (2, 8)), -0.2, 0.2), 0.0, 3.0),
        "velocities": bell_draw(streams_of[1], (3, NTX, NTY, NTZ, SLOTS), 1.0, 6.0, ((1, 4), (2, 8)), jnp.float32),
        "bead_keys": place_ends(jax.random.randint(streams_of[2], (NTX, NTY, NTZ, SLOTS), 0, 1073741824), jax.random.fold_in(streams_of[2], 1), 0, 1073741823).astype(jnp.int32),
        "counts": place_ends(jax.random.randint(streams_of[3], (NTX, NTY, NTZ), SLOTS // 2, SLOTS + 1), jax.random.fold_in(streams_of[3], 1), SLOTS // 2, SLOTS).astype(jnp.int32),
    }


soft_radius = 0.05
friction = 4.5
noise_amplitude = 15.0
like_repulsion = 25.0
unlike_extra = 15.0
kick_scale = 0.02
root_twelve = 3.4641016151377544

def pair_noise(first_keys, second_keys):
    hashed = (first_keys ^ second_keys) * 1103515245 + (first_keys + second_keys) * 12345
    hashed = hashed ^ hashed >> 15 & 131071
    hashed = hashed * 747796405
    hashed = hashed ^ hashed >> 13 & 524287
    fraction = (hashed >> 7 & 16777215).astype(jnp.float32) * (1.0 / 16777216.0)
    return root_twelve * (fraction - 0.5)

def pair_forces(own_motion, own_keys, other_motion, other_keys, other_counts, displace):
    slot_index = lax.broadcasted_iota(jnp.int32, other_keys.shape, 1)
    present = (slot_index < other_counts[:, None]).astype(jnp.float32)
    separation = [own_motion[component][:, :, None] - (other_motion[component][:, None, :] + displace[component]) for component in range(3)]
    squared = separation[0] * separation[0] + separation[1] * separation[1] + separation[2] * separation[2]
    distance = jnp.sqrt(squared)
    weight = jnp.maximum(1.0 - distance, 0.0) * present[:, None, :]
    inverse = 1.0 / jnp.maximum(distance, soft_radius)
    approach = separation[0] * (own_motion[3][:, :, None] - other_motion[3][:, None, :])
    approach = approach + separation[1] * (own_motion[4][:, :, None] - other_motion[4][:, None, :])
    approach = approach + separation[2] * (own_motion[5][:, :, None] - other_motion[5][:, None, :])
    approach = approach * inverse
    first_keys = own_keys[:, :, None]
    second_keys = other_keys[:, None, :]
    random_pair = pair_noise(first_keys, second_keys)
    repulsion = like_repulsion + unlike_extra * ((first_keys ^ second_keys) & 1).astype(jnp.float32)
    strength = (repulsion * weight - friction * weight * weight * approach + noise_amplitude * weight * random_pair) * inverse
    return jnp.stack([lax.optimization_barrier(jnp.sum(strength * part, axis=2)) for part in separation])

def reference(positions, velocities, bead_keys, counts):
    motion = jnp.concatenate([positions, velocities], axis=0)
    size_x, size_y, size_z, slots = bead_keys.shape
    plane = size_y * size_z
    own_motion = jnp.moveaxis(motion, 1, 0).reshape(size_x, 6, plane, slots)
    own_keys = bead_keys.reshape(size_x, plane, slots)
    summed = jnp.zeros((size_x, 3, plane, slots), jnp.float32)
    for off_x in range(3):
        for off_y in range(3):
            for off_z in range(3):
                moved = (1 - off_x, 1 - off_y, 1 - off_z)
                other_motion = jnp.moveaxis(jnp.roll(motion, moved, axis=(1, 2, 3)), 1, 0).reshape(size_x, 6, plane, slots)
                other_keys = jnp.roll(bead_keys, moved, axis=(0, 1, 2)).reshape(size_x, plane, slots)
                other_counts = jnp.roll(counts, moved, axis=(0, 1, 2)).reshape(size_x, plane)
                displace = jnp.array([SIDE * (off_x - 1), SIDE * (off_y - 1), SIDE * (off_z - 1)], jnp.float32)

                def one_plane(items, displace=displace):
                    return pair_forces(items[0], items[1], items[2], items[3], items[4], displace)
                summed = summed + lax.map(one_plane, (own_motion, own_keys, other_motion, other_keys, other_counts))
    slot_index = lax.broadcasted_iota(jnp.int32, bead_keys.shape, 3)
    occupied = (slot_index < counts[:, :, :, None]).astype(jnp.float32)
    force = jnp.moveaxis(summed, 1, 0).reshape(3, size_x, size_y, size_z, slots)
    return kick_scale * force * occupied[None]
```

```python
import functools

import jax
import jax.numpy as jnp
from jax import lax
from jax.experimental import pallas as pl
from jax.experimental.pallas import tpu as pltpu
from jax.sharding import PartitionSpec as P

SIDE = 3.0

soft_radius = 0.05
friction = 4.5
noise_amplitude = 15.0
like_repulsion = 25.0
unlike_extra = 15.0
kick_scale = 0.02
root_twelve = 3.4641016151377544

FAR = 1.0e9
ROWS = 8
GROUP = 64
MESH = pl.DeviceIdType.MESH


def gather_kernel(sizes, pos_ref, vel_ref, key_ref, count_ref, all_ref, packed, send, recv, edge_send, edge_recv, local):
    nx, ny, nz, block_y, tiles_z = sizes
    gx, gy, gz = lax.axis_index("gx"), lax.axis_index("gy"), lax.axis_index("gz")
    slots = pos_ref.shape[-1]
    top = nz * block_y + 1
    barrier = pltpu.get_barrier_semaphore()

    def target(e, group, member):
        return (lax.rem(gx + e + nx, nx), lax.rem(gy + group + ny, ny), lax.rem(member + nz, nz))

    steps = (-1, 0, 1)
    for e in steps:
        for r in range(nz):
            if e or r:
                pl.semaphore_signal(barrier, inc=1, device_id=target(e, 0, gz + r), device_id_type=MESH)
        pl.semaphore_signal(barrier, inc=1, device_id=target(e, -1, nz - 1), device_id_type=MESH)
        pl.semaphore_signal(barrier, inc=1, device_id=target(e, 1, 0), device_id_type=MESH)

    lane = lax.broadcasted_iota(jnp.int32, (1, slots), 1)
    for y in range(block_y):
        for z in range(tiles_z):
            present = lane < count_ref[0, y, z]
            key = key_ref[0, y, pl.ds(z, 1), :]
            rows = [jnp.where(present, pos_ref[c, 0, y, pl.ds(z, 1), :], FAR) for c in range(3)]
            rows += [vel_ref[c, 0, y, pl.ds(z, 1), :] * friction for c in range(3)]
            rows += [(key >> 15).astype(jnp.float32), (key & 32767).astype(jnp.float32)]
            packed[y, z] = jnp.concatenate(rows, axis=0)

    def group_copy(e, r, slot_of):
        return pltpu.make_async_remote_copy(
            src_ref=packed,
            dst_ref=all_ref.at[1 - e, pl.ds(1 + slot_of * block_y, block_y)],
            send_sem=send.at[e + 1, r],
            recv_sem=recv.at[e + 1, r],
            device_id=target(e, 0, gz + r),
            device_id_type=MESH,
        )

    def edge_copy(e, side, member):
        first = side == 0
        return pltpu.make_async_remote_copy(
            src_ref=packed.at[pl.ds(0 if first else block_y - 1, 1)],
            dst_ref=all_ref.at[1 - e, pl.ds(top if first else 0, 1)],
            send_sem=edge_send.at[side, e + 1, member],
            recv_sem=edge_recv.at[side, e + 1],
            device_id=target(e, -1 if first else 1, member),
            device_id_type=MESH,
        )

    ends = jnp.where(gz == 0, 1, 0) + jnp.where(gz == nz - 1, 1, 0)
    pl.semaphore_wait(barrier, 3 * nz - 1 + 3 * nz * ends)

    for e in (-1, 1, 0):
        for r in range(nz):
            if e or r:
                group_copy(e, r, gz).start()

    def edges(side, act):
        for e in (-1, 1, 0):
            for member in range(nz):
                act(edge_copy(e, side, member))

    @pl.when(gz == 0)
    def _():
        edges(0, lambda c: c.start())

    @pl.when(gz == nz - 1)
    def _():
        edges(1, lambda c: c.start())

    mine = pltpu.make_async_copy(packed, all_ref.at[1, pl.ds(1 + gz * block_y, block_y)], local)
    mine.start()
    mine.wait()
    for e in steps:
        for r in range(nz):
            if e or r:
                copy = group_copy(e, r, lax.rem(gz - r + nz, nz))
                copy.wait_recv()
                copy.wait_send()
        for side in range(2):
            edge_copy(e, side, 0).wait_recv()

    @pl.when(gz == 0)
    def _():
        edges(0, lambda c: c.wait_send())

    @pl.when(gz == nz - 1)
    def _():
        edges(1, lambda c: c.wait_send())


def pair_kernel(sizes, all_ref, out_ref, jbuf, column, forces):
    tiles_z, out_y, out_z = sizes
    slots = all_ref.shape[-1]
    gz = lax.axis_index("gz")
    row = lax.broadcasted_iota(jnp.int32, (ROWS, slots), 0)
    lane = lax.broadcasted_iota(jnp.int32, (ROWS, slots), 1)
    low = jnp.where(row < 3, -1.0, -3.0e38)
    high = jnp.where(row < 3, SIDE + 1.0, 3.0e38)

    layers = (0, None) if tiles_z == 2 else (-1, 0, 1)
    shell = [
        (dx, dy, dz)
        for dx in (-1, 0, 1)
        for dy in (-1, 0, 1)
        for dz in layers
        if (dx, dy, dz) != (0, 0, 0)
    ]
    n = len(shell)
    padded_n = -(-n // 8) * 8
    bits = (n * slots - 1).bit_length()
    lane_bits = (slots - 1).bit_length()
    upper = (
        lax.broadcasted_iota(jnp.int32, (slots, slots), 0)
        < lax.broadcasted_iota(jnp.int32, (slots, slots), 1)
    ).astype(jnp.bfloat16)
    below = (
        lax.broadcasted_iota(jnp.int32, (padded_n, padded_n), 1)
        < lax.broadcasted_iota(jnp.int32, (padded_n, padded_n), 0)
    ).astype(jnp.bfloat16)
    flat = lax.broadcasted_iota(jnp.int32, (padded_n, slots), 0) * slots + lax.broadcasted_iota(
        jnp.int32, (padded_n, slots), 1
    )

    def shift(x, bit):
        if bit < lane_bits:
            amount = 1 << bit
            rolled = pltpu.roll(x, slots - amount, 1)
            after = jnp.concatenate([rolled[ROWS:], rolled[:ROWS]], axis=0)
            lanes = lax.broadcasted_iota(jnp.int32, x.shape, 1)
            return jnp.where(lanes < slots - amount, rolled, after)
        cut = ROWS << (bit - lane_bits)
        return jnp.concatenate([x[cut:], x[:cut]], axis=0)

    def one_tile(tile, carry):
        y = tile // out_z
        zz = tile % out_z
        z = gz * out_z + zz
        own = all_ref[1, y + 1, z]
        pieces, masks = [], []
        for dx, dy, dz in shell:
            if dz is None:
                v = all_ref[1 + dx, y + 1 + dy, 1 - z]
                shift_z = jnp.where(v < 0.5 * SIDE, SIDE, -SIDE)
            else:
                v = all_ref[1 + dx, y + 1 + dy, lax.rem(z + dz + tiles_z, tiles_z)]
                shift_z = SIDE * dz
            move = jnp.where(row == 0, SIDE * dx, jnp.where(row == 1, SIDE * dy, jnp.where(row == 2, shift_z, 0.0)))
            v = v + move
            inside = jnp.where((v > low) & (v < high), 1.0, 0.0)
            masks.append(jnp.min(inside, axis=0, keepdims=True))
            pieces.append(v)
        masks += [jnp.zeros((1, slots), jnp.float32)] * (padded_n - n)
        mask = jnp.concatenate(masks, axis=0)
        half = mask.astype(jnp.bfloat16)
        before = jnp.dot(half, upper, preferred_element_type=jnp.float32)
        per_row = jnp.sum(mask, axis=1, keepdims=True)
        rows_before = jnp.dot(
            below,
            jnp.broadcast_to(per_row, (padded_n, slots)).astype(jnp.bfloat16),
            preferred_element_type=jnp.float32,
        )
        total = jnp.sum(mask).astype(jnp.int32)
        distance_left = jnp.where(mask > 0.5, flat - (before + rows_before).astype(jnp.int32), 0)
        x = jnp.concatenate(pieces, axis=0)
        s = jnp.concatenate(
            [jnp.broadcast_to(distance_left[k : k + 1], (ROWS, slots)) for k in range(n)], axis=0
        )
        for bit in range(bits):
            near = shift(s, bit)
            take = (near & (1 << bit)) != 0
            leaves = (s & (1 << bit)) != 0
            x = jnp.where(take, shift(x, bit), x)
            s = jnp.where(take, near, jnp.where(leaves, 0, s))
        jbuf[0] = own
        for k in range(n):
            jbuf[1 + k] = jnp.where(lane + k * slots < total, x[k * ROWS : (k + 1) * ROWS], FAR)
        blocks = 1 + (total + slots - 1) // slots

        column[:, :ROWS] = jnp.transpose(own)
        count = jnp.sum(jnp.where(own[0:1] < 0.5 * FAR, 1.0, 0.0)).astype(jnp.int32)
        groups = (count + GROUP - 1) // GROUP

        def one_group(g, carry):
            base = pl.multiple_of(g * GROUP, GROUP)

            def wide(c):
                return jnp.broadcast_to(column[pl.ds(base, GROUP), c : c + 1], (GROUP, slots))

            xi = [wide(c) for c in range(6)]
            klo = wide(7).astype(jnp.int32)
            ki = wide(6).astype(jnp.int32) * 32768 + klo
            ai = ki * 12345
            ti = (klo & 1).astype(jnp.float32) * unlike_extra - 0.5 * unlike_extra

            def one_block(b, acc):
                def other(c):
                    return jbuf[b, pl.ds(c, 1), :]

                sep = [xi[c] - other(c) for c in range(3)]
                squared = sep[0] * sep[0] + sep[1] * sep[1] + sep[2] * sep[2]
                distance = squared * lax.rsqrt(jnp.maximum(squared, 1e-30))
                inverse = lax.rsqrt(jnp.maximum(squared, soft_radius * soft_radius))
                weight = jnp.maximum(1.0 - distance, 0.0)
                dot = (
                    sep[0] * (xi[3] - other(3))
                    + sep[1] * (xi[4] - other(4))
                    + sep[2] * (xi[5] - other(5))
                )
                lo = other(7).astype(jnp.int32)
                kj = other(6).astype(jnp.int32) * 32768 + lo
                tj = 1.0 - 2.0 * (lo & 1).astype(jnp.float32)
                hashed = (ki ^ kj) * 1103515245 + (ai + kj * 12345)
                hashed = hashed ^ lax.shift_right_logical(hashed, 15)
                hashed = hashed * 747796405
                hashed = hashed ^ lax.shift_right_logical(hashed, 13)
                fraction = (lax.shift_right_logical(hashed, 7) & 16777215).astype(jnp.float32)
                unit = noise_amplitude * root_twelve
                push = (
                    fraction * (unit / 16777216.0)
                    + (like_repulsion + 0.5 * unlike_extra - 0.5 * unit)
                    + ti * tj
                )
                scaled = weight * inverse
                strength = scaled * (push - scaled * dot)
                return tuple(acc[c] + strength * sep[c] for c in range(3))

            zero = jnp.zeros((GROUP, slots), jnp.float32)
            acc = lax.fori_loop(0, blocks, one_block, (zero, zero, zero))
            lanes = lax.broadcasted_iota(jnp.int32, (GROUP, slots), 1)
            sums = [jnp.sum(a, axis=1, keepdims=True) for a in acc]
            forces[pl.ds(base, GROUP), :] = jnp.where(
                lanes == 0, sums[0], jnp.where(lanes == 1, sums[1], sums[2])
            )
            return carry

        lax.fori_loop(0, groups, one_group, 0)
        turned = jnp.transpose(forces[...])
        kick = jnp.where(lane[:3] < count, kick_scale * turned[:3], 0.0)
        for c in range(3):
            out_ref[c, 0, y, pl.ds(zz, 1), :] = kick[c : c + 1]
        return carry

    lax.fori_loop(0, out_y * out_z, one_tile, 0)


def on_device(nx, ny, nz, positions, velocities, bead_keys, counts):
    _, _, block_y, tiles_z, slots = positions.shape
    out_y, out_z = block_y * nz, tiles_z // nz
    span = out_y + 2
    gathered = pl.pallas_call(
        functools.partial(gather_kernel, (nx, ny, nz, block_y, tiles_z)),
        out_shape=jax.ShapeDtypeStruct((3, span, tiles_z, ROWS, slots), jnp.float32),
        in_specs=[pl.BlockSpec(memory_space=pltpu.VMEM)] * 3 + [pl.BlockSpec(memory_space=pltpu.SMEM)],
        out_specs=pl.BlockSpec(memory_space=pltpu.VMEM),
        scratch_shapes=[
            pltpu.VMEM((block_y, tiles_z, ROWS, slots), jnp.float32),
            pltpu.SemaphoreType.DMA((3, nz)),
            pltpu.SemaphoreType.DMA((3, nz)),
            pltpu.SemaphoreType.DMA((2, 3, nz)),
            pltpu.SemaphoreType.DMA((2, 3)),
            pltpu.SemaphoreType.DMA,
        ],
        compiler_params=pltpu.CompilerParams(collective_id=0, has_side_effects=True),
        name="gather_tiles",
    )(positions, velocities, bead_keys, counts)
    shells = 17 if tiles_z == 2 else 26
    return pl.pallas_call(
        functools.partial(pair_kernel, (tiles_z, out_y, out_z)),
        out_shape=jax.ShapeDtypeStruct((3, 1, out_y, out_z, slots), jnp.float32),
        in_specs=[pl.BlockSpec(memory_space=pltpu.VMEM)],
        out_specs=pl.BlockSpec(memory_space=pltpu.VMEM),
        scratch_shapes=[
            pltpu.VMEM((1 + shells, ROWS, slots), jnp.float32),
            pltpu.VMEM((slots, slots), jnp.float32),
            pltpu.VMEM((slots, slots), jnp.float32),
        ],
        name="pair_kicks",
    )(gathered)


def solution(mesh):
    in_specs = (
        P(None, "gx", ("gy", "gz"), None, None),
        P(None, "gx", ("gy", "gz"), None, None),
        P("gx", ("gy", "gz"), None, None),
        P("gx", ("gy", "gz"), None),
    )
    out_specs = P(None, "gx", "gy", "gz", None)
    nx, ny, nz = mesh.shape["gx"], mesh.shape["gy"], mesh.shape["gz"]
    return jax.shard_map(
        functools.partial(on_device, nx, ny, nz),
        mesh=mesh,
        in_specs=in_specs,
        out_specs=out_specs,
        check_vma=False,
    )
```

```python
import functools

import jax
import jax.numpy as jnp
from jax import lax
from jax.experimental import pallas as pl
from jax.experimental.pallas import tpu as pltpu
from jax.sharding import PartitionSpec as P

SIDE = 3.0

soft_radius = 0.05
friction = 4.5
noise_amplitude = 15.0
like_repulsion = 25.0
unlike_extra = 15.0
kick_scale = 0.02
root_twelve = 3.4641016151377544

FAR = 1.0e9
ROWS = 8
GROUP = 64
MESH = pl.DeviceIdType.MESH


def gather_kernel(sizes, pos_ref, vel_ref, key_ref, count_ref, all_ref, packed, send, recv, edge_send, edge_recv, local):
    nx, ny, nz, block_y, tiles_z = sizes
    gx, gy, gz = lax.axis_index("gx"), lax.axis_index("gy"), lax.axis_index("gz")
    slots = pos_ref.shape[-1]
    top = nz * block_y + 1
    barrier = pltpu.get_barrier_semaphore()

    def target(e, group, member):
        return (lax.rem(gx + e + nx, nx), lax.rem(gy + group + ny, ny), lax.rem(member + nz, nz))

    steps = (-1, 0, 1)
    for e in steps:
        for r in range(nz):
            if e or r:
                pl.semaphore_signal(barrier, inc=1, device_id=target(e, 0, gz + r), device_id_type=MESH)
        pl.semaphore_signal(barrier, inc=1, device_id=target(e, -1, nz - 1), device_id_type=MESH)
        pl.semaphore_signal(barrier, inc=1, device_id=target(e, 1, 0), device_id_type=MESH)

    lane = lax.broadcasted_iota(jnp.int32, (1, slots), 1)
    for y in range(block_y):
        for z in range(tiles_z):
            present = lane < count_ref[0, z, y]
            key = key_ref[0, y, pl.ds(z, 1), :]
            rows = [jnp.where(present, pos_ref[c, 0, y, pl.ds(z, 1), :], FAR) for c in range(3)]
            rows += [vel_ref[c, 0, y, pl.ds(z, 1), :] * friction for c in range(3)]
            rows += [(key >> 15).astype(jnp.float32), (key & 32767).astype(jnp.float32)]
            packed[y, z] = jnp.concatenate(rows, axis=0)

    def group_copy(e, r, slot_of):
        return pltpu.make_async_remote_copy(
            src_ref=packed,
            dst_ref=all_ref.at[1 - e, pl.ds(1 + slot_of * block_y, block_y)],
            send_sem=send.at[e + 1, r],
            recv_sem=recv.at[e + 1, r],
            device_id=target(e, 0, gz + r),
            device_id_type=MESH,
        )

    def edge_copy(e, side, member):
        first = side == 0
        return pltpu.make_async_remote_copy(
            src_ref=packed.at[pl.ds(0 if first else block_y - 1, 1)],
            dst_ref=all_ref.at[1 - e, pl.ds(top if first else 0, 1)],
            send_sem=edge_send.at[side, e + 1, member],
            recv_sem=edge_recv.at[side, e + 1],
            device_id=target(e, -1 if first else 1, member),
            device_id_type=MESH,
        )

    ends = jnp.where(gz == 0, 1, 0) + jnp.where(gz == nz - 1, 1, 0)
    pl.semaphore_wait(barrier, 3 * nz - 1 + 3 * nz * ends)

    for e in (-1, 1, 0):
        for r in range(nz):
            if e or r:
                group_copy(e, r, gz).start()

    def edges(side, act):
        for e in (-1, 1, 0):
            for member in range(nz):
                act(edge_copy(e, side, member))

    @pl.when(gz == 0)
    def _():
        edges(0, lambda c: c.start())

    @pl.when(gz == nz - 1)
    def _():
        edges(1, lambda c: c.start())

    mine = pltpu.make_async_copy(packed, all_ref.at[1, pl.ds(1 + gz * block_y, block_y)], local)
    mine.start()
    mine.wait()
    for e in steps:
        for r in range(nz):
            if e or r:
                copy = group_copy(e, r, lax.rem(gz - r + nz, nz))
                copy.wait_recv()
                copy.wait_send()
        for side in range(2):
            edge_copy(e, side, 0).wait_recv()

    @pl.when(gz == 0)
    def _():
        edges(0, lambda c: c.wait_send())

    @pl.when(gz == nz - 1)
    def _():
        edges(1, lambda c: c.wait_send())


def shell_of(tiles_z):
    layers = (0, None) if tiles_z == 2 else (-1, 0, 1)
    offsets = [(dx, dy, dz) for dx in (-1, 0, 1) for dy in (-1, 0, 1) for dz in layers]
    return [offset for offset in offsets if offset != (0, 0, 0)]


def pair_kernel(sizes, all_ref, out_ref, jbuf, column, forces, masks, places, sources, moved, limits):
    tiles_z, out_y, out_z = sizes
    slots = all_ref.shape[-1]
    tiles = out_y * out_z
    gz = lax.axis_index("gz")
    row = lax.broadcasted_iota(jnp.int32, (ROWS, slots), 0)
    lane = lax.broadcasted_iota(jnp.int32, (ROWS, slots), 1)
    low = jnp.where(row < 3, -1.0, -3.0e38)
    high = jnp.where(row < 3, SIDE + 1.0, 3.0e38)
    shell = shell_of(tiles_z)
    n = len(shell)
    padded_n = masks.shape[0] // tiles

    def candidate(k, y, z):
        dx, dy, dz = shell[k]
        if dz is None:
            v = all_ref[1 + dx, y + 1 + dy, 1 - z]
            shift_z = jnp.where(v < 0.5 * SIDE, SIDE, -SIDE)
        else:
            v = all_ref[1 + dx, y + 1 + dy, lax.rem(z + dz + tiles_z, tiles_z)]
            shift_z = SIDE * dz
        return v + jnp.where(
            row == 0, SIDE * dx, jnp.where(row == 1, SIDE * dy, jnp.where(row == 2, shift_z, 0.0))
        )

    def mark(tile, carry):
        y, z = tile // out_z, gz * out_z + tile % out_z
        rows = []
        for k in range(n):
            v = candidate(k, y, z)
            inside = jnp.where((v > low) & (v < high), 1.0, 0.0)
            rows.append(jnp.min(inside, axis=0, keepdims=True))
        rows += [jnp.zeros((1, slots), jnp.float32)] * (padded_n - n)
        masks[pl.ds(pl.multiple_of(tile * padded_n, 8), padded_n), :] = jnp.concatenate(rows, axis=0)
        return carry

    lax.fori_loop(0, tiles, mark, 0)

    def square(size, test):
        i = lax.broadcasted_iota(jnp.int32, (size, size), 0)
        j = lax.broadcasted_iota(jnp.int32, (size, size), 1)
        return jnp.where(test(i, j), 1.0, 0.0).astype(jnp.bfloat16)

    height = tiles * padded_n
    mask = masks[...]
    half = mask.astype(jnp.bfloat16)
    rank = jnp.dot(half, square(slots, lambda i, j: i < j), preferred_element_type=jnp.float32)
    inside = jnp.dot(half, jnp.ones((slots, slots), jnp.bfloat16), preferred_element_type=jnp.float32)
    start = jnp.concatenate(
        [
            jnp.dot(
                square(padded_n, lambda i, j: j < i),
                inside[t * padded_n : (t + 1) * padded_n].astype(jnp.bfloat16),
                preferred_element_type=jnp.float32,
            )
            for t in range(tiles)
        ],
        axis=0,
    ).astype(jnp.int32)
    inside = inside.astype(jnp.int32)
    lanes = lax.broadcasted_iota(jnp.int32, (height, slots), 1)
    left = jnp.where(mask > 0.5, lanes - rank.astype(jnp.int32), 0)
    lane_bits = (slots - 1).bit_length()
    for bit in range(lane_bits):
        near = pltpu.roll(left, slots - (1 << bit), 1)
        take = (near & (1 << bit)) != 0
        leaves = (left & (1 << bit)) != 0
        left = jnp.where(take, near, jnp.where(leaves, 0, left))
    source = lanes + left
    for bit in range(lane_bits):
        source = jnp.where((start & (1 << bit)) != 0, pltpu.roll(source, 1 << bit, 1), source)
    offset = (lanes - start) & (slots - 1)
    sources[...] = source & (slots - 1)
    places[...] = jnp.where(offset < inside, (start + offset) >> lane_bits, -1)
    ends = start + inside
    for t in range(tiles):
        last = t * padded_n + n - 1
        limits[0, t] = jnp.max(ends[last : last + 1])
        own_x = all_ref[1, 1 + t // out_z, gz * out_z + t % out_z, pl.ds(0, 1), :]
        limits[1, t] = jnp.sum(jnp.where(own_x < 0.5 * FAR, 1.0, 0.0)).astype(jnp.int32)

    def one_tile(tile, carry):
        y, zz = tile // out_z, tile % out_z
        z = gz * out_z + zz
        own = all_ref[1, y + 1, z]
        first = tile * padded_n
        for k in range(n):
            index = jnp.broadcast_to(sources[pl.ds(first + k, 1), :], (ROWS, slots))
            moved[k] = jnp.take_along_axis(candidate(k, y, z), index, axis=1, mode="promise_in_bounds")
        blocks = 1 + (limits[0, tile] + slots - 1) // slots
        count = limits[1, tile]
        jbuf[0] = own

        def fill(b, carry):
            block = jnp.full((ROWS, slots), FAR, jnp.float32)
            for k in range(n):
                block = jnp.where(places[pl.ds(first + k, 1), :] == b - 1, moved[k], block)
            jbuf[b] = block
            return carry

        lax.fori_loop(1, blocks, fill, 0)
        column[:, :ROWS] = jnp.transpose(own)
        groups = (count + GROUP - 1) // GROUP

        def one_group(g, carry):
            base = pl.multiple_of(g * GROUP, GROUP)

            def wide(c):
                return jnp.broadcast_to(column[pl.ds(base, GROUP), c : c + 1], (GROUP, slots))

            xi = [wide(c) for c in range(6)]
            klo = wide(7).astype(jnp.int32)
            ki = wide(6).astype(jnp.int32) * 32768 + klo
            ai = ki * 12345
            ti = (klo & 1).astype(jnp.float32) * unlike_extra - 0.5 * unlike_extra

            def one_block(b, acc):
                def other(c):
                    return jbuf[b, pl.ds(c, 1), :]

                sep = [xi[c] - other(c) for c in range(3)]
                squared = sep[0] * sep[0] + sep[1] * sep[1] + sep[2] * sep[2]
                distance = squared * lax.rsqrt(jnp.maximum(squared, 1e-30))
                inverse = lax.rsqrt(jnp.maximum(squared, soft_radius * soft_radius))
                weight = jnp.maximum(1.0 - distance, 0.0)
                dot = (
                    sep[0] * (xi[3] - other(3))
                    + sep[1] * (xi[4] - other(4))
                    + sep[2] * (xi[5] - other(5))
                )
                lo = other(7).astype(jnp.int32)
                kj = other(6).astype(jnp.int32) * 32768 + lo
                tj = 1.0 - 2.0 * (lo & 1).astype(jnp.float32)
                hashed = (ki ^ kj) * 1103515245 + (ai + kj * 12345)
                hashed = hashed ^ lax.shift_right_logical(hashed, 15)
                hashed = hashed * 747796405
                hashed = hashed ^ lax.shift_right_logical(hashed, 13)
                fraction = (lax.shift_right_logical(hashed, 7) & 16777215).astype(jnp.float32)
                unit = noise_amplitude * root_twelve
                push = (
                    fraction * (unit / 16777216.0)
                    + (like_repulsion + 0.5 * unlike_extra - 0.5 * unit)
                    + ti * tj
                )
                scaled = weight * inverse
                strength = scaled * (push - scaled * dot)
                return tuple(acc[c] + strength * sep[c] for c in range(3))

            zero = jnp.zeros((GROUP, slots), jnp.float32)
            acc = lax.fori_loop(0, blocks, one_block, (zero, zero, zero))
            lanes = lax.broadcasted_iota(jnp.int32, (GROUP, slots), 1)
            sums = [jnp.sum(a, axis=1, keepdims=True) for a in acc]
            forces[pl.ds(base, GROUP), :] = jnp.where(
                lanes == 0, sums[0], jnp.where(lanes == 1, sums[1], sums[2])
            )
            return carry

        lax.fori_loop(0, groups, one_group, 0)
        turned = jnp.transpose(forces[...])
        kick = jnp.where(lane[:3] < count, kick_scale * turned[:3], 0.0)
        for c in range(3):
            out_ref[c, 0, y, pl.ds(zz, 1), :] = kick[c : c + 1]
        return carry

    lax.fori_loop(0, tiles, one_tile, 0)


def on_device(nx, ny, nz, positions, velocities, bead_keys, counts):
    _, _, block_y, tiles_z, slots = positions.shape
    out_y, out_z = block_y * nz, tiles_z // nz
    span = out_y + 2
    gathered = pl.pallas_call(
        functools.partial(gather_kernel, (nx, ny, nz, block_y, tiles_z)),
        out_shape=jax.ShapeDtypeStruct((3, span, tiles_z, ROWS, slots), jnp.float32),
        in_specs=[pl.BlockSpec(memory_space=pltpu.VMEM)] * 3 + [pl.BlockSpec(memory_space=pltpu.SMEM)],
        out_specs=pl.BlockSpec(memory_space=pltpu.VMEM),
        scratch_shapes=[
            pltpu.VMEM((block_y, tiles_z, ROWS, slots), jnp.float32),
            pltpu.SemaphoreType.DMA((3, nz)),
            pltpu.SemaphoreType.DMA((3, nz)),
            pltpu.SemaphoreType.DMA((2, 3, nz)),
            pltpu.SemaphoreType.DMA((2, 3)),
            pltpu.SemaphoreType.DMA,
        ],
        compiler_params=pltpu.CompilerParams(collective_id=0, has_side_effects=True),
        name="gather_tiles",
    )(positions, velocities, bead_keys, jnp.swapaxes(counts, 1, 2))
    shells = len(shell_of(tiles_z))
    height = out_y * out_z * (-(-shells // 8) * 8)
    return pl.pallas_call(
        functools.partial(pair_kernel, (tiles_z, out_y, out_z)),
        out_shape=jax.ShapeDtypeStruct((3, 1, out_y, out_z, slots), jnp.float32),
        in_specs=[pl.BlockSpec(memory_space=pltpu.VMEM)],
        out_specs=pl.BlockSpec(memory_space=pltpu.VMEM),
        scratch_shapes=[
            pltpu.VMEM((1 + shells, ROWS, slots), jnp.float32),
            pltpu.VMEM((slots, slots), jnp.float32),
            pltpu.VMEM((slots, slots), jnp.float32),
            pltpu.VMEM((height, slots), jnp.float32),
            pltpu.VMEM((height, slots), jnp.int32),
            pltpu.VMEM((height, slots), jnp.int32),
            pltpu.VMEM((shells, ROWS, slots), jnp.float32),
            pltpu.SMEM((2, out_y * out_z), jnp.int32),
        ],
        name="pair_kicks",
    )(gathered)


def solution(mesh):
    in_specs = (
        P(None, "gx", ("gy", "gz"), None, None),
        P(None, "gx", ("gy", "gz"), None, None),
        P("gx", ("gy", "gz"), None, None),
        P("gx", ("gy", "gz"), None),
    )
    out_specs = P(None, "gx", "gy", "gz", None)
    nx, ny, nz = mesh.shape["gx"], mesh.shape["gy"], mesh.shape["gz"]
    return jax.shard_map(
        functools.partial(on_device, nx, ny, nz),
        mesh=mesh,
        in_specs=in_specs,
        out_specs=out_specs,
        check_vma=False,
    )
```

```python
import functools

import jax
import jax.numpy as jnp
from jax import lax
from jax.experimental import pallas as pl
from jax.experimental.pallas import tpu as pltpu
from jax.sharding import PartitionSpec as P

SIDE = 3.0

soft_radius = 0.05
friction = 4.5
noise_amplitude = 15.0
like_repulsion = 25.0
unlike_extra = 15.0
kick_scale = 0.02
root_twelve = 3.4641016151377544

FAR = 1.0e9
ROWS = 8
GROUP = 128
MESH = pl.DeviceIdType.MESH


def gather_kernel(sizes, pos_in, vel_in, key_in, count_in, all_ref, pos_ref, vel_ref, key_ref, count_ref, packed, send, recv, edge_send, edge_recv, local, loads):
    nx, ny, nz, block_y, tiles_z = sizes
    gx, gy, gz = lax.axis_index("gx"), lax.axis_index("gy"), lax.axis_index("gz")
    slots = pos_ref.shape[-1]
    inputs = ((pos_in, pos_ref), (vel_in, vel_ref), (key_in, key_ref), (count_in, count_ref))
    fetches = [pltpu.make_async_copy(a, b, loads.at[k]) for k, (a, b) in enumerate(inputs)]
    for fetch in fetches:
        fetch.start()
    top = nz * block_y + 1
    barrier = pltpu.get_barrier_semaphore()

    def target(e, group, member):
        return (lax.rem(gx + e + nx, nx), lax.rem(gy + group + ny, ny), lax.rem(member + nz, nz))

    steps = (-1, 0, 1)
    for e in steps:
        for r in range(nz):
            if e or r:
                pl.semaphore_signal(barrier, inc=1, device_id=target(e, 0, gz + r), device_id_type=MESH)
        pl.semaphore_signal(barrier, inc=1, device_id=target(e, -1, nz - 1), device_id_type=MESH)
        pl.semaphore_signal(barrier, inc=1, device_id=target(e, 1, 0), device_id_type=MESH)

    for fetch in fetches:
        fetch.wait()
    lane = lax.broadcasted_iota(jnp.int32, (1, slots), 1)
    for y in range(block_y):
        for z in range(tiles_z):
            present = lane < count_ref[0, z, y]
            key = key_ref[0, y, pl.ds(z, 1), :]
            rows = [jnp.where(present, pos_ref[c, 0, y, pl.ds(z, 1), :], FAR) for c in range(3)]
            rows += [vel_ref[c, 0, y, pl.ds(z, 1), :] * friction for c in range(3)]
            rows += [(key >> 15).astype(jnp.float32), (key & 32767).astype(jnp.float32)]
            packed[y, z] = jnp.concatenate(rows, axis=0)

    def group_copy(e, r, slot_of):
        return pltpu.make_async_remote_copy(
            src_ref=packed,
            dst_ref=all_ref.at[1 - e, pl.ds(1 + slot_of * block_y, block_y)],
            send_sem=send.at[e + 1, r],
            recv_sem=recv.at[e + 1, r],
            device_id=target(e, 0, gz + r),
            device_id_type=MESH,
        )

    def edge_copy(e, side, member):
        first = side == 0
        return pltpu.make_async_remote_copy(
            src_ref=packed.at[pl.ds(0 if first else block_y - 1, 1)],
            dst_ref=all_ref.at[1 - e, pl.ds(top if first else 0, 1)],
            send_sem=edge_send.at[side, e + 1, member],
            recv_sem=edge_recv.at[side, e + 1],
            device_id=target(e, -1 if first else 1, member),
            device_id_type=MESH,
        )

    ends = jnp.where(gz == 0, 1, 0) + jnp.where(gz == nz - 1, 1, 0)
    pl.semaphore_wait(barrier, 3 * nz - 1 + 3 * nz * ends)

    for e in (-1, 1, 0):
        for r in range(nz):
            if e or r:
                group_copy(e, r, gz).start()

    def edges(side, act):
        for e in (-1, 1, 0):
            for member in range(nz):
                act(edge_copy(e, side, member))

    @pl.when(gz == 0)
    def _():
        edges(0, lambda c: c.start())

    @pl.when(gz == nz - 1)
    def _():
        edges(1, lambda c: c.start())

    mine = pltpu.make_async_copy(packed, all_ref.at[1, pl.ds(1 + gz * block_y, block_y)], local)
    mine.start()
    mine.wait()
    for e in steps:
        for r in range(nz):
            if e or r:
                copy = group_copy(e, r, lax.rem(gz - r + nz, nz))
                copy.wait_recv()
                copy.wait_send()
        for side in range(2):
            edge_copy(e, side, 0).wait_recv()

    @pl.when(gz == 0)
    def _():
        edges(0, lambda c: c.wait_send())

    @pl.when(gz == nz - 1)
    def _():
        edges(1, lambda c: c.wait_send())


def shell_of(tiles_z):
    layers = (0, None) if tiles_z == 2 else (-1, 0, 1)
    offsets = [(dx, dy, dz) for dx in (-1, 0, 1) for dy in (-1, 0, 1) for dz in layers]
    return [offset for offset in offsets if offset != (0, 0, 0)]


def pair_kernel(sizes, all_ref, out_ref, jbuf, column, forces, masks, places, sources, moved, limits):
    tiles_z, out_y, out_z = sizes
    slots = all_ref.shape[-1]
    tiles = out_y * out_z
    gz = lax.axis_index("gz")
    row = lax.broadcasted_iota(jnp.int32, (ROWS, slots), 0)
    lane = lax.broadcasted_iota(jnp.int32, (ROWS, slots), 1)
    low = jnp.where(row < 3, -1.0, -3.0e38)
    high = jnp.where(row < 3, SIDE + 1.0, 3.0e38)
    shell = shell_of(tiles_z)
    n = len(shell)
    padded_n = masks.shape[0] // tiles

    def candidate(k, y, z):
        dx, dy, dz = shell[k]
        if dz is None:
            v = all_ref[1 + dx, y + 1 + dy, 1 - z]
            shift_z = jnp.where(v < 0.5 * SIDE, SIDE, -SIDE)
        else:
            v = all_ref[1 + dx, y + 1 + dy, lax.rem(z + dz + tiles_z, tiles_z)]
            shift_z = SIDE * dz
        return v + jnp.where(
            row == 0, SIDE * dx, jnp.where(row == 1, SIDE * dy, jnp.where(row == 2, shift_z, 0.0))
        )

    def mark(tile, carry):
        y, z = tile // out_z, gz * out_z + tile % out_z
        rows = []
        for k in range(n):
            v = candidate(k, y, z)
            inside = jnp.where((v > low) & (v < high), 1.0, 0.0)
            rows.append(jnp.min(inside, axis=0, keepdims=True))
        rows += [jnp.zeros((1, slots), jnp.float32)] * (padded_n - n)
        masks[pl.ds(pl.multiple_of(tile * padded_n, 8), padded_n), :] = jnp.concatenate(rows, axis=0)
        return carry

    lax.fori_loop(0, tiles, mark, 0, unroll=2)

    def square(size, test):
        i = lax.broadcasted_iota(jnp.int32, (size, size), 0)
        j = lax.broadcasted_iota(jnp.int32, (size, size), 1)
        return jnp.where(test(i, j), 1.0, 0.0).astype(jnp.bfloat16)

    height = tiles * padded_n
    mask = masks[...]
    half = mask.astype(jnp.bfloat16)
    rank = jnp.dot(half, square(slots, lambda i, j: i < j), preferred_element_type=jnp.float32)
    inside = jnp.dot(half, jnp.ones((slots, slots), jnp.bfloat16), preferred_element_type=jnp.float32)
    start = jnp.concatenate(
        [
            jnp.dot(
                square(padded_n, lambda i, j: j < i),
                inside[t * padded_n : (t + 1) * padded_n].astype(jnp.bfloat16),
                preferred_element_type=jnp.float32,
            )
            for t in range(tiles)
        ],
        axis=0,
    ).astype(jnp.int32)
    inside = inside.astype(jnp.int32)
    lanes = lax.broadcasted_iota(jnp.int32, (height, slots), 1)
    left = jnp.where(mask > 0.5, lanes - rank.astype(jnp.int32), 0)
    lane_bits = (slots - 1).bit_length()
    for bit in range(lane_bits):
        near = pltpu.roll(left, slots - (1 << bit), 1)
        take = (near & (1 << bit)) != 0
        leaves = (left & (1 << bit)) != 0
        left = jnp.where(take, near, jnp.where(leaves, 0, left))
    source = lanes + left
    for bit in range(lane_bits):
        source = jnp.where((start & (1 << bit)) != 0, pltpu.roll(source, 1 << bit, 1), source)
    offset = (lanes - start) & (slots - 1)
    sources[...] = source & (slots - 1)
    places[...] = jnp.where(offset < inside, (start + offset) >> lane_bits, -1)
    ends = start + inside
    for t in range(tiles):
        last = t * padded_n + n - 1
        limits[0, t] = jnp.max(ends[last : last + 1])
        own_x = all_ref[1, 1 + t // out_z, gz * out_z + t % out_z, pl.ds(0, 1), :]
        limits[1, t] = jnp.sum(jnp.where(own_x < 0.5 * FAR, 1.0, 0.0)).astype(jnp.int32)

    def collect(tile, carry):
        y, z = tile // out_z, gz * out_z + tile % out_z
        first = tile * padded_n
        for k in range(n):
            index = jnp.broadcast_to(sources[pl.ds(first + k, 1), :], (ROWS, slots))
            moved[tile, k] = jnp.take_along_axis(candidate(k, y, z), index, axis=1, mode="promise_in_bounds")
        column[tile, :, :ROWS] = jnp.transpose(all_ref[1, y + 1, z])
        return carry

    lax.fori_loop(0, tiles, collect, 0, unroll=2)

    def one_tile(tile, carry):
        y, zz = tile // out_z, tile % out_z
        z = gz * out_z + zz
        own = all_ref[1, y + 1, z]
        first = tile * padded_n
        blocks = 1 + (limits[0, tile] + slots - 1) // slots
        count = limits[1, tile]
        jbuf[0] = own

        def fill(b, carry):
            block = jnp.full((ROWS, slots), FAR, jnp.float32)
            for k in range(n):
                block = jnp.where(places[pl.ds(first + k, 1), :] == b - 1, moved[tile, k], block)
            jbuf[b] = block
            return carry

        lax.fori_loop(1, blocks, fill, 0)
        groups = (count + GROUP - 1) // GROUP

        def one_group(g, carry):
            base = pl.multiple_of(g * GROUP, GROUP)

            def wide(c):
                return jnp.broadcast_to(column[tile, pl.ds(base, GROUP), c : c + 1], (GROUP, slots))

            xi = [wide(c) for c in range(6)]
            klo = wide(7).astype(jnp.int32)
            ki = wide(6).astype(jnp.int32) * 32768 + klo
            ai = ki * 12345
            ti = (klo & 1).astype(jnp.float32) * unlike_extra - 0.5 * unlike_extra

            def one_block(b, acc):
                def other(c):
                    return jbuf[b, pl.ds(c, 1), :]

                sep = [xi[c] - other(c) for c in range(3)]
                squared = sep[0] * sep[0] + sep[1] * sep[1] + sep[2] * sep[2]
                root = lax.rsqrt(jnp.maximum(squared, 1e-30))
                distance = squared * root
                inverse = jnp.minimum(root, 1.0 / soft_radius)
                weight = jnp.maximum(1.0 - distance, 0.0)
                dot = (
                    sep[0] * (xi[3] - other(3))
                    + sep[1] * (xi[4] - other(4))
                    + sep[2] * (xi[5] - other(5))
                )
                lo = other(7).astype(jnp.int32)
                kj = other(6).astype(jnp.int32) * 32768 + lo
                tj = 1.0 - 2.0 * (lo & 1).astype(jnp.float32)
                hashed = (ki ^ kj) * 1103515245 + (ai + kj * 12345)
                hashed = hashed ^ lax.shift_right_logical(hashed, 15)
                hashed = hashed * 747796405
                hashed = hashed ^ lax.shift_right_logical(hashed, 13)
                fraction = (lax.shift_right_logical(hashed, 7) & 16777215).astype(jnp.float32)
                unit = noise_amplitude * root_twelve
                push = (
                    fraction * (unit / 16777216.0)
                    + (like_repulsion + 0.5 * unlike_extra - 0.5 * unit)
                    + ti * tj
                )
                scaled = weight * inverse
                strength = scaled * (push - scaled * dot)
                return tuple(acc[c] + strength * sep[c] for c in range(3))

            zero = jnp.zeros((GROUP, slots), jnp.float32)
            acc = lax.fori_loop(0, blocks, one_block, (zero, zero, zero))
            for c in range(3):
                forces[tile, c, pl.ds(base, GROUP), :] = acc[c]
            return carry

        lax.fori_loop(0, groups, one_group, 0)
        return carry

    lax.fori_loop(0, tiles, one_tile, 0)

    def finish(tile, carry):
        lanes = lax.broadcasted_iota(jnp.int32, (slots, slots), 1)
        sums = [jnp.sum(forces[tile, c], axis=1, keepdims=True) for c in range(3)]
        turned = jnp.transpose(jnp.where(lanes == 0, sums[0], jnp.where(lanes == 1, sums[1], sums[2])))
        kick = jnp.where(lane[:3] < limits[1, tile], kick_scale * turned[:3], 0.0)
        for c in range(3):
            out_ref[c, 0, tile // out_z, pl.ds(tile % out_z, 1), :] = kick[c : c + 1]
        return carry

    lax.fori_loop(0, tiles, finish, 0, unroll=2)


def on_device(nx, ny, nz, positions, velocities, bead_keys, counts):
    _, _, block_y, tiles_z, slots = positions.shape
    out_y, out_z = block_y * nz, tiles_z // nz
    span = out_y + 2
    gathered = pl.pallas_call(
        functools.partial(gather_kernel, (nx, ny, nz, block_y, tiles_z)),
        out_shape=jax.ShapeDtypeStruct((3, span, tiles_z, ROWS, slots), jnp.float32),
        in_specs=[pl.BlockSpec(memory_space=pltpu.HBM)] * 4,
        out_specs=pl.BlockSpec(memory_space=pl.ANY),
        scratch_shapes=[
            pltpu.VMEM(positions.shape, jnp.float32),
            pltpu.VMEM(velocities.shape, jnp.float32),
            pltpu.VMEM(bead_keys.shape, jnp.int32),
            pltpu.SMEM((1, tiles_z, block_y), jnp.int32),
            pltpu.VMEM((block_y, tiles_z, ROWS, slots), jnp.float32),
            pltpu.SemaphoreType.DMA((3, nz)),
            pltpu.SemaphoreType.DMA((3, nz)),
            pltpu.SemaphoreType.DMA((2, 3, nz)),
            pltpu.SemaphoreType.DMA((2, 3)),
            pltpu.SemaphoreType.DMA,
            pltpu.SemaphoreType.DMA((4,)),
        ],
        compiler_params=pltpu.CompilerParams(
            collective_id=0, has_side_effects=True, vmem_limit_bytes=8 << 20
        ),
        name="gather_tiles",
    )(positions, velocities, bead_keys, jnp.swapaxes(counts, 1, 2))
    shells = len(shell_of(tiles_z))
    height = out_y * out_z * (-(-shells // 8) * 8)
    return pl.pallas_call(
        functools.partial(pair_kernel, (tiles_z, out_y, out_z)),
        out_shape=jax.ShapeDtypeStruct((3, 1, out_y, out_z, slots), jnp.float32),
        in_specs=[pl.BlockSpec(memory_space=pltpu.VMEM)],
        out_specs=pl.BlockSpec(memory_space=pltpu.VMEM),
        scratch_shapes=[
            pltpu.VMEM((1 + shells, ROWS, slots), jnp.float32),
            pltpu.VMEM((out_y * out_z, slots, slots), jnp.float32),
            pltpu.VMEM((out_y * out_z, 3, slots, slots), jnp.float32),
            pltpu.VMEM((height, slots), jnp.float32),
            pltpu.VMEM((height, slots), jnp.int32),
            pltpu.VMEM((height, slots), jnp.int32),
            pltpu.VMEM((out_y * out_z, shells, ROWS, slots), jnp.float32),
            pltpu.SMEM((2, out_y * out_z), jnp.int32),
        ],
        compiler_params=pltpu.CompilerParams(vmem_limit_bytes=8 << 20),
        name="pair_kicks",
    )(gathered)


def solution(mesh):
    in_specs = (
        P(None, "gx", ("gy", "gz"), None, None),
        P(None, "gx", ("gy", "gz"), None, None),
        P("gx", ("gy", "gz"), None, None),
        P("gx", ("gy", "gz"), None),
    )
    out_specs = P(None, "gx", "gy", "gz", None)
    nx, ny, nz = mesh.shape["gx"], mesh.shape["gy"], mesh.shape["gz"]
    return jax.shard_map(
        functools.partial(on_device, nx, ny, nz),
        mesh=mesh,
        in_specs=in_specs,
        out_specs=out_specs,
        check_vma=False,
    )
```

```python
import functools

import jax
import jax.numpy as jnp
from jax import lax
from jax.experimental import pallas as pl
from jax.experimental.pallas import tpu as pltpu
from jax.sharding import PartitionSpec as P

SIDE = 3.0

soft_radius = 0.05
friction = 4.5
noise_amplitude = 15.0
like_repulsion = 25.0
unlike_extra = 15.0
kick_scale = 0.02
root_twelve = 3.4641016151377544

FAR = 1.0e9
ROWS = 8
GROUP = 128
MESH = pl.DeviceIdType.MESH


def gather_kernel(sizes, pos_in, vel_in, key_in, count_in, all_ref, pos_ref, vel_ref, key_ref, count_ref, packed, send, recv, edge_send, edge_recv, local, loads):
    nx, ny, nz, block_y, tiles_z = sizes
    gx, gy, gz = lax.axis_index("gx"), lax.axis_index("gy"), lax.axis_index("gz")
    slots = pos_ref.shape[-1]
    inputs = ((pos_in, pos_ref), (vel_in, vel_ref), (key_in, key_ref), (count_in, count_ref))
    fetches = [pltpu.make_async_copy(a, b, loads.at[k]) for k, (a, b) in enumerate(inputs)]
    for fetch in fetches:
        fetch.start()
    top = nz * block_y + 1
    barrier = pltpu.get_barrier_semaphore()

    def target(e, group, member):
        return (lax.rem(gx + e + nx, nx), lax.rem(gy + group + ny, ny), lax.rem(member + nz, nz))

    steps = (-1, 0, 1)
    for e in steps:
        for r in range(nz):
            if e or r:
                pl.semaphore_signal(barrier, inc=1, device_id=target(e, 0, gz + r), device_id_type=MESH)
        pl.semaphore_signal(barrier, inc=1, device_id=target(e, -1, nz - 1), device_id_type=MESH)
        pl.semaphore_signal(barrier, inc=1, device_id=target(e, 1, 0), device_id_type=MESH)

    for fetch in fetches:
        fetch.wait()
    lane = lax.broadcasted_iota(jnp.int32, (1, slots), 1)
    for y in range(block_y):
        for z in range(tiles_z):
            present = lane < count_ref[0, z, y]
            key = key_ref[0, y, pl.ds(z, 1), :]
            rows = [jnp.where(present, pos_ref[c, 0, y, pl.ds(z, 1), :], FAR) for c in range(3)]
            rows += [vel_ref[c, 0, y, pl.ds(z, 1), :] * friction for c in range(3)]
            rows += [(key >> 15).astype(jnp.float32), (key & 32767).astype(jnp.float32)]
            packed[y, z] = jnp.concatenate(rows, axis=0)

    def group_copy(e, r, slot_of):
        return pltpu.make_async_remote_copy(
            src_ref=packed,
            dst_ref=all_ref.at[1 - e, pl.ds(1 + slot_of * block_y, block_y)],
            send_sem=send.at[e + 1, r],
            recv_sem=recv.at[e + 1, r],
            device_id=target(e, 0, gz + r),
            device_id_type=MESH,
        )

    def edge_copy(e, side, member):
        first = side == 0
        return pltpu.make_async_remote_copy(
            src_ref=packed.at[pl.ds(0 if first else block_y - 1, 1)],
            dst_ref=all_ref.at[1 - e, pl.ds(top if first else 0, 1)],
            send_sem=edge_send.at[side, e + 1, member],
            recv_sem=edge_recv.at[side, e + 1],
            device_id=target(e, -1 if first else 1, member),
            device_id_type=MESH,
        )

    ends = jnp.where(gz == 0, 1, 0) + jnp.where(gz == nz - 1, 1, 0)
    pl.semaphore_wait(barrier, 3 * nz - 1 + 3 * nz * ends)

    for e in (-1, 1, 0):
        for r in range(nz):
            if e or r:
                group_copy(e, r, gz).start()

    def edges(side, act):
        for e in (-1, 1, 0):
            for member in range(nz):
                act(edge_copy(e, side, member))

    @pl.when(gz == 0)
    def _():
        edges(0, lambda c: c.start())

    @pl.when(gz == nz - 1)
    def _():
        edges(1, lambda c: c.start())

    mine = pltpu.make_async_copy(packed, all_ref.at[1, pl.ds(1 + gz * block_y, block_y)], local)
    mine.start()
    mine.wait()
    for e in steps:
        for r in range(nz):
            if e or r:
                copy = group_copy(e, r, lax.rem(gz - r + nz, nz))
                copy.wait_recv()
                copy.wait_send()
        for side in range(2):
            edge_copy(e, side, 0).wait_recv()

    @pl.when(gz == 0)
    def _():
        edges(0, lambda c: c.wait_send())

    @pl.when(gz == nz - 1)
    def _():
        edges(1, lambda c: c.wait_send())


def shell_of(tiles_z):
    layers = (0, None) if tiles_z == 2 else (-1, 0, 1)
    offsets = [(dx, dy, dz) for dx in (-1, 0, 1) for dy in (-1, 0, 1) for dz in layers]
    return [offset for offset in offsets if offset != (0, 0, 0)]


def pair_kernel(sizes, all_ref, out_ref, jbuf, column, forces, masks, places, sources, moved, limits):
    tiles_z, out_y, out_z = sizes
    slots = all_ref.shape[-1]
    tiles = out_y * out_z
    gz = lax.axis_index("gz")
    row = lax.broadcasted_iota(jnp.int32, (ROWS, slots), 0)
    lane = lax.broadcasted_iota(jnp.int32, (ROWS, slots), 1)
    low = jnp.where(row < 3, -1.0, -3.0e38)
    high = jnp.where(row < 3, SIDE + 1.0, 3.0e38)
    shell = shell_of(tiles_z)
    n = len(shell)
    padded_n = masks.shape[0] // tiles

    def candidate(k, y, z):
        dx, dy, dz = shell[k]
        if dz is None:
            v = all_ref[1 + dx, y + 1 + dy, 1 - z]
            shift_z = jnp.where(v < 0.5 * SIDE, SIDE, -SIDE)
        else:
            v = all_ref[1 + dx, y + 1 + dy, lax.rem(z + dz + tiles_z, tiles_z)]
            shift_z = SIDE * dz
        return v + jnp.where(
            row == 0, SIDE * dx, jnp.where(row == 1, SIDE * dy, jnp.where(row == 2, shift_z, 0.0))
        )

    def mark(tile, carry):
        y, z = tile // out_z, gz * out_z + tile % out_z
        rows = []
        for k in range(n):
            v = candidate(k, y, z)
            inside = jnp.where((v > low) & (v < high), 1.0, 0.0)
            rows.append(jnp.min(inside, axis=0, keepdims=True))
        rows += [jnp.zeros((1, slots), jnp.float32)] * (padded_n - n)
        masks[pl.ds(pl.multiple_of(tile * padded_n, 8), padded_n), :] = jnp.concatenate(rows, axis=0)
        return carry

    lax.fori_loop(0, tiles, mark, 0, unroll=2)

    def square(size, test):
        i = lax.broadcasted_iota(jnp.int32, (size, size), 0)
        j = lax.broadcasted_iota(jnp.int32, (size, size), 1)
        return jnp.where(test(i, j), 1.0, 0.0).astype(jnp.bfloat16)

    height = tiles * padded_n
    mask = masks[...]
    half = mask.astype(jnp.bfloat16)
    rank = jnp.dot(half, square(slots, lambda i, j: i < j), preferred_element_type=jnp.float32)
    inside = jnp.dot(half, jnp.ones((slots, slots), jnp.bfloat16), preferred_element_type=jnp.float32)
    start = jnp.concatenate(
        [
            jnp.dot(
                square(padded_n, lambda i, j: j < i),
                inside[t * padded_n : (t + 1) * padded_n].astype(jnp.bfloat16),
                preferred_element_type=jnp.float32,
            )
            for t in range(tiles)
        ],
        axis=0,
    ).astype(jnp.int32)
    inside = inside.astype(jnp.int32)
    lanes = lax.broadcasted_iota(jnp.int32, (height, slots), 1)
    left = jnp.where(mask > 0.5, lanes - rank.astype(jnp.int32), 0)
    lane_bits = (slots - 1).bit_length()
    for bit in range(lane_bits):
        near = pltpu.roll(left, slots - (1 << bit), 1)
        take = (near & (1 << bit)) != 0
        leaves = (left & (1 << bit)) != 0
        left = jnp.where(take, near, jnp.where(leaves, 0, left))
    source = lanes + left
    for bit in range(lane_bits):
        source = jnp.where((start & (1 << bit)) != 0, pltpu.roll(source, 1 << bit, 1), source)
    offset = (lanes - start) & (slots - 1)
    sources[...] = source & (slots - 1)
    places[...] = jnp.where(offset < inside, (start + offset) >> lane_bits, -1)
    ends = start + inside
    for t in range(tiles):
        last = t * padded_n + n - 1
        limits[0, t] = jnp.max(ends[last : last + 1])
        own_x = all_ref[1, 1 + t // out_z, gz * out_z + t % out_z, pl.ds(0, 1), :]
        limits[1, t] = jnp.sum(jnp.where(own_x < 0.5 * FAR, 1.0, 0.0)).astype(jnp.int32)

    def collect(tile, carry):
        y, z = tile // out_z, gz * out_z + tile % out_z
        first = tile * padded_n
        for k in range(n):
            index = jnp.broadcast_to(sources[pl.ds(first + k, 1), :], (ROWS, slots))
            moved[tile, k] = jnp.take_along_axis(candidate(k, y, z), index, axis=1, mode="promise_in_bounds")
        column[tile, :, :ROWS] = jnp.transpose(all_ref[1, y + 1, z])
        return carry

    lax.fori_loop(0, tiles, collect, 0, unroll=2)

    def one_tile(tile, carry):
        y, zz = tile // out_z, tile % out_z
        z = gz * out_z + zz
        own = all_ref[1, y + 1, z]
        first = tile * padded_n
        blocks = 1 + (limits[0, tile] + slots - 1) // slots
        count = limits[1, tile]
        jbuf[0] = own

        def fill(b, carry):
            block = jnp.full((ROWS, slots), FAR, jnp.float32)
            for k in range(n):
                block = jnp.where(places[pl.ds(first + k, 1), :] == b - 1, moved[tile, k], block)
            jbuf[b] = block
            return carry

        lax.fori_loop(1, blocks, fill, 0)
        groups = (count + GROUP - 1) // GROUP

        def one_group(g, carry):
            base = pl.multiple_of(g * GROUP, GROUP)

            def wide(c):
                return jnp.broadcast_to(column[tile, pl.ds(base, GROUP), c : c + 1], (GROUP, slots))

            xi = [wide(c) for c in range(6)]
            klo = wide(7).astype(jnp.int32)
            ki = wide(6).astype(jnp.int32) * 32768 + klo
            ai = ki * 12345
            ti = (klo & 1).astype(jnp.float32) * unlike_extra - 0.5 * unlike_extra

            def one_block(b, acc):
                def other(c):
                    return jbuf[b, pl.ds(c, 1), :]

                sep = [xi[c] - other(c) for c in range(3)]
                squared = sep[0] * sep[0] + sep[1] * sep[1] + sep[2] * sep[2]
                root = lax.rsqrt(jnp.maximum(squared, 1e-30))
                distance = squared * root
                inverse = jnp.minimum(root, 1.0 / soft_radius)
                weight = jnp.maximum(1.0 - distance, 0.0)
                dot = (
                    sep[0] * (xi[3] - other(3))
                    + sep[1] * (xi[4] - other(4))
                    + sep[2] * (xi[5] - other(5))
                )
                lo = other(7).astype(jnp.int32)
                kj = other(6).astype(jnp.int32) * 32768 + lo
                tj = 1.0 - 2.0 * (lo & 1).astype(jnp.float32)
                hashed = (ki ^ kj) * 1103515245 + (ai + kj * 12345)
                hashed = hashed ^ lax.shift_right_logical(hashed, 15)
                hashed = hashed * 747796405
                hashed = hashed ^ lax.shift_right_logical(hashed, 13)
                fraction = (lax.shift_right_logical(hashed, 7) & 16777215).astype(jnp.float32)
                unit = noise_amplitude * root_twelve
                push = (
                    fraction * (unit / 16777216.0)
                    + (like_repulsion + 0.5 * unlike_extra - 0.5 * unit)
                    + ti * tj
                )
                scaled = weight * inverse
                strength = scaled * (push - scaled * dot)
                return tuple(acc[c] + strength * sep[c] for c in range(3))

            zero = jnp.zeros((GROUP, slots), jnp.float32)
            acc = lax.fori_loop(0, blocks, one_block, (zero, zero, zero))
            for c in range(3):
                forces[tile, c, pl.ds(base, GROUP), :] = acc[c]
            return carry

        lax.fori_loop(0, groups, one_group, 0)
        return carry

    lax.fori_loop(0, tiles, one_tile, 0)

    def finish(tile, carry):
        lanes = lax.broadcasted_iota(jnp.int32, (slots, slots), 1)
        sums = [jnp.sum(forces[tile, c], axis=1, keepdims=True) for c in range(3)]
        turned = jnp.transpose(jnp.where(lanes == 0, sums[0], jnp.where(lanes == 1, sums[1], sums[2])))
        kick = jnp.where(lane[:3] < limits[1, tile], kick_scale * turned[:3], 0.0)
        for c in range(3):
            out_ref[c, 0, tile // out_z, pl.ds(tile % out_z, 1), :] = kick[c : c + 1]
        return carry

    lax.fori_loop(0, tiles, finish, 0, unroll=2)


def on_device(nx, ny, nz, positions, velocities, bead_keys, counts):
    _, _, block_y, tiles_z, slots = positions.shape
    out_y, out_z = block_y * nz, tiles_z // nz
    span = out_y + 2
    gathered = pl.pallas_call(
        functools.partial(gather_kernel, (nx, ny, nz, block_y, tiles_z)),
        out_shape=jax.ShapeDtypeStruct((3, span, tiles_z, ROWS, slots), jnp.float32),
        in_specs=[pl.BlockSpec(memory_space=pltpu.HBM)] * 4,
        out_specs=pl.BlockSpec(memory_space=pl.ANY),
        scratch_shapes=[
            pltpu.VMEM(positions.shape, jnp.float32),
            pltpu.VMEM(velocities.shape, jnp.float32),
            pltpu.VMEM(bead_keys.shape, jnp.int32),
            pltpu.SMEM((1, tiles_z, block_y), jnp.int32),
            pltpu.VMEM((block_y, tiles_z, ROWS, slots), jnp.float32),
            pltpu.SemaphoreType.DMA((3, nz)),
            pltpu.SemaphoreType.DMA((3, nz)),
            pltpu.SemaphoreType.DMA((2, 3, nz)),
            pltpu.SemaphoreType.DMA((2, 3)),
            pltpu.SemaphoreType.DMA,
            pltpu.SemaphoreType.DMA((4,)),
        ],
        compiler_params=pltpu.CompilerParams(
            collective_id=0, has_side_effects=True
        ),
        name="gather_tiles",
    )(positions, velocities, bead_keys, jnp.swapaxes(counts, 1, 2))
    shells = len(shell_of(tiles_z))
    height = out_y * out_z * (-(-shells // 8) * 8)
    return pl.pallas_call(
        functools.partial(pair_kernel, (tiles_z, out_y, out_z)),
        out_shape=jax.ShapeDtypeStruct((3, 1, out_y, out_z, slots), jnp.float32),
        in_specs=[pl.BlockSpec(memory_space=pltpu.VMEM)],
        out_specs=pl.BlockSpec(memory_space=pltpu.VMEM),
        scratch_shapes=[
            pltpu.VMEM((1 + shells, ROWS, slots), jnp.float32),
            pltpu.VMEM((out_y * out_z, slots, slots), jnp.float32),
            pltpu.VMEM((out_y * out_z, 3, slots, slots), jnp.float32),
            pltpu.VMEM((height, slots), jnp.float32),
            pltpu.VMEM((height, slots), jnp.int32),
            pltpu.VMEM((height, slots), jnp.int32),
            pltpu.VMEM((out_y * out_z, shells, ROWS, slots), jnp.float32),
            pltpu.SMEM((2, out_y * out_z), jnp.int32),
        ],
        name="pair_kicks",
    )(gathered)


def solution(mesh):
    in_specs = (
        P(None, "gx", ("gy", "gz"), None, None),
        P(None, "gx", ("gy", "gz"), None, None),
        P("gx", ("gy", "gz"), None, None),
        P("gx", ("gy", "gz"), None),
    )
    out_specs = P(None, "gx", "gy", "gz", None)
    nx, ny, nz = mesh.shape["gx"], mesh.shape["gy"], mesh.shape["gz"]
    return jax.shard_map(
        functools.partial(on_device, nx, ny, nz),
        mesh=mesh,
        in_specs=in_specs,
        out_specs=out_specs,
        check_vma=False,
    )
```
